32 devices in a mesh: sub: 8 (over z, x), tile: 4 (over y, core).
Axes of the slice: x: 2, y: 2, z: 4, core: 2. Of those that a mesh axis runs over, the one named last changes fastest.
Arguments:
- coupling: bfloat16 [8, 28, 256, 256], P('sub'), may hold values from -0.125 to 0.125
- panel_inv: float32 [8, 8, 256, 256], P('sub')
- a_ib: bfloat16 [8, 2048, 3072], P('sub', None, 'tile'), may hold values from -0.5 to 0.5
- owner: int32 [8, 12, 12], P('sub', None, 'tile'), may hold values from 0 to 7, as said below
- slot: int32 [8, 12, 12], P('sub', None, 'tile'), may hold values from 0 to 15
- base: bfloat16 [8, 64, 256, 256], P('sub', 'tile'), may hold values from -2 to 2
Outputs:
- assembled: bfloat16 [8, 64, 256, 256], P('sub', 'tile')
The draws below stay inside these ranges and needn't reach their ends.
Inputs may be any that keep to these rules, and one draw needn't show every extreme that they name: `owner`: tiles of one device are those of one subdomain s and tile columns t*12/4 to (t+1)*12/4 - 1. At most 5 tiles of one device name one sub index; for each t one sub index, drawn from the seed, is named by exactly 5 tiles of every device of that t.
All inputs are finite; a program needn't handle non-finite values.
Results may differ from the reference program's by a relative error of at most 0.0051.
Values may be sent and summed in bfloat16 or wider, within the bound.
A program may use at most 128 MiB of HBM per device.

```python
import math
import jax
import jax.numpy as jnp
from jax import lax

NI = 2048
NB = 3072
PANEL = 256
SLOTS = 16
LOWER = 28
NBT = 12
SUBS = 8
OWNED = 64
N_SUB = 8
N_TILE = 4


def draw_panel_inv(key, part):
    random_key = jax.random.fold_in(key, 1)
    shape = (SUBS, NI // PANEL, PANEL, PANEL)
    random_part = jax.random.normal(random_key, shape, jnp.float32)
    identity = jnp.eye(PANEL, dtype=jnp.float32)
    return 0.6 * identity + 0.3 * random_part / math.sqrt(PANEL)


def draw_owner(key, part):
    tile_side = NB // PANEL
    tile_count = tile_side * tile_side // N_TILE
    capacity = (tile_count + N_SUB - 1) // N_SUB
    others = (N_SUB - 1) * capacity
    hot_key, seat_key = jax.random.split(key)
    hottest = jax.random.randint(hot_key, (N_TILE,), 0, N_SUB).astype(jnp.int32)

    def one_device(device_key, hot_owner):
        first_key, second_key = jax.random.split(device_key)
        seat_order = jax.random.permutation(first_key, others)[:tile_count - capacity].astype(jnp.int32)
        chosen = (hot_owner + 1 + seat_order // capacity) % N_SUB
        listed = jnp.concatenate([jnp.full((capacity,), hot_owner, jnp.int32), chosen.astype(jnp.int32)])
        return listed[jax.random.permutation(second_key, tile_count)]
    device_keys = jax.random.split(seat_key, SUBS * N_TILE)
    hot_all = jnp.tile(hottest, SUBS)
    drawn = jax.vmap(one_device)(device_keys, hot_all)
    drawn = drawn.reshape(SUBS, N_TILE, tile_side, tile_count // tile_side)
    return drawn.transpose(0, 2, 1, 3).reshape(SUBS, tile_side, tile_side)


def set_ends(array, rng, least, high):
    extent = array.shape
    index_at = [jax.random.randint(jax.random.fold_in(rng, axis), (), 0, extent[axis]) for axis in range(len(extent))]
    array = array.at[tuple(index_at)].set(least)
    longest = extent.index(max(extent))
    index_at[longest] = (index_at[longest] + 1) % extent[longest]
    return array.at[tuple(index_at)].set(high)


def level_of(stream_key, dims, cuts, low, top_value):
    loudness, own = 1.0, jax.random.fold_in(stream_key, 6)
    for axis_at, parts in cuts:
        steps = jnp.exp(jax.random.uniform(jax.random.fold_in(own, axis_at), (parts,), jnp.float32, low / len(cuts), top_value / len(cuts)))
        loudness = loudness * jnp.repeat(steps, dims[axis_at] // parts).reshape([-1 if axis == axis_at else 1 for axis in range(len(dims))])
    return loudness


def scatter_about(key, shape, scale, most, pieces=(), kind=jnp.bfloat16):
    values = scale * jax.random.normal(key, shape, jnp.float32)
    if pieces:
        values = values * level_of(key, shape, pieces, -0.22, 0.18)
    return jnp.clip(values, -most, most).astype(kind)


def setup_inputs(seed: int = 0) -> dict:
    key_of = jax.random.split(jax.random.key(seed), 7)
    coupling = scatter_about(key_of[0], (SUBS, LOWER, PANEL, PANEL), NI ** -0.5, 0.125, ((0, 8),))
    panel_inv = draw_panel_inv(jax.random.fold_in(key_of[6], 71), 0)
    a_ib = scatter_about(key_of[2], (SUBS, NI, NB), 0.0625, 0.5, ((0, 8), (2, 4)))
    owner = draw_owner(jax.random.fold_in(key_of[6], 71), 0)
    slot = set_ends(jax.random.randint(key_of[4], (SUBS, NBT, NBT), 0, SLOTS), jax.random.fold_in(key_of[4], 1), 0, SLOTS - 1).astype(jnp.int32)
    base = scatter_about(key_of[5], (SUBS, OWNED, PANEL, PANEL), 0.3, 2.0, ((0, 8), (1, 4)))
    return dict(coupling=coupling, panel_inv=panel_inv, a_ib=a_ib, owner=owner, slot=slot, base=base)


def solve(lower_blocks, inverse, right_cols):
    panel_width = inverse.shape[1]
    panels = []
    for row_panel in range(inverse.shape[0]):
        target = right_cols[row_panel * panel_width:(row_panel + 1) * panel_width].astype(jnp.float32)
        if row_panel > 0:
            block_start = row_panel * (row_panel - 1) // 2
            blocks = lower_blocks[block_start:block_start + row_panel]
            joined = jnp.transpose(blocks, (1, 0, 2)).reshape(panel_width, row_panel * panel_width)
            target = target - jnp.dot(joined, jnp.concatenate(panels, axis=0), preferred_element_type=jnp.float32)
        solved_panel = jnp.dot(inverse[row_panel], target, precision=lax.Precision.HIGHEST, preferred_element_type=jnp.float32)
        panels.append(solved_panel.astype(jnp.bfloat16))
    return jnp.concatenate(panels, axis=0)


def reference(coupling, panel_inv, a_ib, owner, slot, base):
    tile_side = NB // PANEL
    col_tiles = tile_side // N_TILE
    column_group = jnp.arange(tile_side, dtype=jnp.int32) // col_tiles

    def assemble_one(accumulated, operands):
        lower_blocks, inverse, right_cols, owner_ids, slot_ids = operands
        solved = solve(lower_blocks, inverse, right_cols)
        gram_matrix = lax.dot_general(solved, solved, (((0,), (0,)), ((), ())), preferred_element_type=jnp.float32)
        contrib = (-gram_matrix).astype(jnp.bfloat16)
        contrib = lax.optimization_barrier(contrib).astype(jnp.float32)
        tiled = contrib.reshape(tile_side, PANEL, tile_side, PANEL).transpose(0, 2, 1, 3)
        places = column_group[None, :] * SLOTS + slot_ids
        accumulated = accumulated.at[owner_ids, places].add(tiled)
        return accumulated, None

    start_total = jnp.zeros((SUBS, OWNED, PANEL, PANEL), jnp.float32)
    accumulated, _ = lax.scan(assemble_one, start_total, (coupling, panel_inv, a_ib, owner, slot))
    return (base.astype(jnp.float32) + accumulated).astype(jnp.bfloat16)
```

```python
import functools

import jax
import jax.numpy as jnp
from jax import lax
from jax.experimental import pallas as pl
from jax.experimental.pallas import tpu as pltpu
from jax.sharding import PartitionSpec as P

MESH = pl.DeviceIdType.MESH
F32 = jnp.float32
BF16 = jnp.bfloat16


def exchange_kernel(
    dims,
    meta_sm,
    meta_any,
    coupling_hbm,
    inverse_hbm,
    cols_hbm,
    incoming,
    metas,
    labels,
    coupling,
    inverse,
    cols,
    target,
    held,
    total,
    packed,
    table,
    meta_all,
    load_sem,
    own_send,
    own_recv,
    relay_send,
    relay_recv,
    out_send,
    out_recv,
    meta_send,
    meta_recv,
    local_sem,
):
    n_sub, n_tile, panels, width, col_tiles, tile_count, capacity, slots = dims
    me = lax.axis_index("sub")
    col = lax.axis_index("tile")
    half_tile = n_tile // 2
    partner = col + 1 - 2 * (col % 2)
    across = (col + half_tile) % n_tile
    corner = (partner + half_tile) % n_tile
    places = (col, partner, across, corner)
    half = n_sub // 2
    side = me // half
    within = me % half

    def far_peer(j):
        return ((side + 1) % 2) * half + (within + j) % half

    def near_peer(j):
        return side * half + (within + j) % half

    loads = [
        pltpu.make_async_copy(cols_hbm.at[0], cols.at[0], load_sem.at[0]),
        pltpu.make_async_copy(inverse_hbm.at[0], inverse.at[0], load_sem.at[1]),
        pltpu.make_async_copy(coupling_hbm, coupling, load_sem.at[2]),
        pltpu.make_async_copy(
            inverse_hbm.at[pl.ds(1, panels - 1)], inverse.at[pl.ds(1, panels - 1)], load_sem.at[3]
        ),
        pltpu.make_async_copy(
            cols_hbm.at[pl.ds(1, panels - 1)], cols.at[pl.ds(1, panels - 1)], load_sem.at[4]
        ),
    ]
    for load in loads:
        load.start()

    barrier = pltpu.get_barrier_semaphore()
    for place in (partner, across):
        pl.semaphore_signal(barrier, inc=1, device_id={"tile": place}, device_id_type=MESH)

    @pl.loop(1, n_sub)
    def _(j):
        pl.semaphore_signal(
            barrier, inc=1, device_id={"sub": (me + j) % n_sub}, device_id_type=MESH
        )

    def solve_panel(k):
        target[...] = cols[k].astype(F32)
        start = k * (k - 1) // 2
        for m in range(k):
            target[...] -= jnp.dot(coupling[start + m], held[m], preferred_element_type=F32)
        inv = inverse[k]
        inv_high = inv.astype(BF16)
        inv_low = (inv - inv_high.astype(F32)).astype(BF16)
        value = target[...]
        high = value.astype(BF16)
        low = (value - high.astype(F32)).astype(BF16)
        answer = jnp.dot(inv_high, low, preferred_element_type=F32)
        answer += jnp.dot(inv_low, high, preferred_element_type=F32)
        answer += jnp.dot(inv_high, high, preferred_element_type=F32)
        held[k] = answer.astype(BF16)

    def own_copy(k, way):
        return pltpu.make_async_remote_copy(
            src_ref=held.at[k],
            dst_ref=held.at[(way + 1) * panels + k],
            send_sem=own_send.at[way, k],
            recv_sem=own_recv.at[way, k],
            device_id={"tile": (partner, across)[way]},
            device_id_type=MESH,
        )

    def relay_copy(k):
        return pltpu.make_async_remote_copy(
            src_ref=held.at[2 * panels + k],
            dst_ref=held.at[3 * panels + k],
            send_sem=relay_send.at[k],
            recv_sem=relay_recv.at[k],
            device_id={"tile": partner},
            device_id_type=MESH,
        )

    def out_copy(peer, source):
        return pltpu.make_async_remote_copy(
            src_ref=packed.at[peer],
            dst_ref=incoming.at[source],
            send_sem=out_send.at[peer],
            recv_sem=out_recv.at[source],
            device_id={"sub": peer},
            device_id_type=MESH,
        )

    def meta_copy(peer, source):
        return pltpu.make_async_remote_copy(
            src_ref=meta_any,
            dst_ref=metas.at[source],
            send_sem=meta_send.at[peer],
            recv_sem=meta_recv.at[source],
            device_id={"sub": peer},
            device_id_type=MESH,
        )

    loads[0].wait()
    loads[1].wait()
    solve_panel(0)
    pl.semaphore_wait(barrier, n_sub + 1)
    own_copy(0, 1).start()
    own_copy(0, 0).start()
    for load in loads[2:]:
        load.wait()
    for k in range(1, panels):
        solve_panel(k)
        own_copy(k, 1).start()
        own_copy(k, 0).start()

    @pl.loop(1, n_sub)
    def _(j):
        meta_copy((me + j) % n_sub, me).start()

    per_place = col_tiles * col_tiles

    def gram(u, k, first=False):
        right = held[k]
        for i in range(col_tiles):
            left = held[u * panels + k, :, i * width : (i + 1) * width]
            product = lax.dot_general(
                left, right, (((0,), (0,)), ((), ())), preferred_element_type=F32
            )
            for j in range(col_tiles):
                piece = product[:, j * width : (j + 1) * width]
                at = places[u] * per_place + i * col_tiles + j
                if first:
                    total[at] = piece
                else:
                    total[at] += piece

    def pick(read, low, default, value_of, store):
        def body(i, carry):
            count, chosen = carry
            value = read(i)
            hit = (value >= low) & (value < low + slots)
            new = value_of(i, value)
            chosen = tuple(
                jnp.where(hit & (count == r), new, c) for r, c in enumerate(chosen)
            )
            return count + jnp.where(hit, 1, 0), chosen

        start = (jnp.int32(0), tuple(jnp.int32(default) for _ in range(capacity)))
        _, chosen = lax.fori_loop(0, tile_count, body, start)
        for r, c in enumerate(chosen):
            store(r, c)

    @pl.loop(0, n_sub)
    def _(d):
        def store(r, c):
            table[d * capacity + r] = c

        pick(lambda i: meta_sm[0, i], d * slots, 0, lambda i, v: i, store)

    gram(0, 0, first=True)

    @pl.loop(1, panels)
    def _(k):
        gram(0, k)

    own_copy(0, 0).wait_recv()
    gram(1, 0, first=True)

    @pl.loop(1, panels)
    def _(k):
        own_copy(k, 0).wait_recv()
        gram(1, k)

    def remote_step(k, first):
        own_copy(k, 1).wait_recv()
        relay_copy(k).start()
        gram(2, k, first)
        relay_copy(k).wait_recv()
        gram(3, k, first)

    remote_step(0, True)

    @pl.loop(1, panels)
    def _(k):
        remote_step(k, False)

    def pack(d):
        for r in range(capacity):
            packed[d, r] = (-total[table[d * capacity + r]]).astype(BF16)

    @pl.loop(0, half)
    def _(j):
        pack(far_peer(j))
        out_copy(far_peer(j), me).start()

    @pl.loop(1, half)
    def _(j):
        pack(near_peer(j))
        out_copy(near_peer(j), me).start()

    pack(me)
    keep = pltpu.make_async_copy(packed.at[me], incoming.at[me], local_sem.at[0])
    keep.start()

    own_meta = pltpu.make_async_copy(meta_any, meta_all.at[me], local_sem.at[1])
    own_meta.start()

    @pl.loop(1, n_sub)
    def _(j):
        source = (me + j) % n_sub
        meta_copy(source, source).wait_recv()
        fetch = pltpu.make_async_copy(metas.at[source], meta_all.at[source], local_sem.at[2])
        fetch.start()
        fetch.wait()

    own_meta.wait()

    @pl.loop(0, n_sub)
    def _(s):
        def store(r, c):
            labels[s * capacity + r] = c

        pick(
            lambda i: meta_all[s, 0, i], me * slots, slots, lambda i, v: v - me * slots, store
        )

    @pl.loop(0, panels)
    def _(k):
        own_copy(k, 0).wait_send()
        own_copy(k, 1).wait_send()
        relay_copy(k).wait_send()

    @pl.loop(1, n_sub)
    def _(j):
        source = (me + j) % n_sub
        meta_copy(source, source).wait_send()
        out_copy(source, source).wait_send()
        out_copy(source, source).wait_recv()

    keep.wait()


def add_kernel(slots, capacity, labels, incoming, base, result, total):
    step = pl.program_id(0)

    @pl.when(step == 0)
    def _():
        total[pl.ds(0, slots)] = base[...].astype(F32)

    for r in range(capacity):
        total[labels[step * capacity + r]] += incoming[0, r].astype(F32)

    @pl.when(step == pl.num_programs(0) - 1)
    def _():
        result[...] = total[pl.ds(0, slots)].astype(BF16)


def shards(coupling, panel_inv, a_ib, owner, slot, base):
    lower_blocks = coupling[0]
    inverse = panel_inv[0]
    panels, width = inverse.shape[:2]
    col_count = a_ib.shape[2]
    right_cols = a_ib[0].reshape(panels, width, col_count)
    n_sub = lax.axis_size("sub")
    n_tile = lax.axis_size("tile")
    assert n_tile == 4 and n_sub % 2 == 0
    col_tiles = col_count // width
    tile_count = owner.shape[1] * owner.shape[2]
    assert owner.shape[1] == n_tile * col_tiles
    capacity = (tile_count + n_sub - 1) // n_sub
    slots = base.shape[1]
    room = (tile_count + 127) // 128 * 128
    meta = (owner[0] * slots + slot[0]).reshape(1, tile_count)
    meta = jnp.pad(meta, ((0, 0), (0, room - tile_count)))
    dims = (n_sub, n_tile, panels, width, col_tiles, tile_count, capacity, slots)
    any_spec = pl.BlockSpec(memory_space=pl.ANY)
    smem_spec = pl.BlockSpec(memory_space=pltpu.SMEM)
    dma = pltpu.SemaphoreType.DMA
    incoming, _, labels = pl.pallas_call(
        functools.partial(exchange_kernel, dims),
        out_shape=(
            jax.ShapeDtypeStruct((n_sub, capacity, width, width), BF16),
            jax.ShapeDtypeStruct((n_sub, 1, room), jnp.int32),
            jax.ShapeDtypeStruct((n_sub * capacity,), jnp.int32),
        ),
        in_specs=[smem_spec, any_spec, any_spec, any_spec, any_spec],
        out_specs=(any_spec, any_spec, smem_spec),
        scratch_shapes=[
            pltpu.VMEM(lower_blocks.shape, BF16),
            pltpu.VMEM(inverse.shape, F32),
            pltpu.VMEM(right_cols.shape, BF16),
            pltpu.VMEM((width, col_count), F32),
            pltpu.VMEM((n_tile * panels, width, col_count), BF16),
            pltpu.VMEM((tile_count, width, width), F32),
            pltpu.VMEM((n_sub, capacity, width, width), BF16),
            pltpu.SMEM((n_sub * capacity,), jnp.int32),
            pltpu.SMEM((n_sub, 1, room), jnp.int32),
            dma((5,)),
            dma((2, panels)),
            dma((2, panels)),
            dma((panels,)),
            dma((panels,)),
            dma((n_sub,)),
            dma((n_sub,)),
            dma((n_sub,)),
            dma((n_sub,)),
            dma((3,)),
        ],
        compiler_params=pltpu.CompilerParams(
            collective_id=0, has_side_effects=True, vmem_limit_bytes=60 * 1024 * 1024
        ),
    )(meta, meta, lower_blocks, inverse, right_cols)

    whole_block = pl.BlockSpec((slots, width, width), lambda s: (0, 0, 0))
    result = pl.pallas_call(
        functools.partial(add_kernel, slots, capacity),
        grid=(n_sub,),
        out_shape=jax.ShapeDtypeStruct((slots, width, width), BF16),
        in_specs=[
            smem_spec,
            pl.BlockSpec((1, capacity, width, width), lambda s: (s, 0, 0, 0)),
            whole_block,
        ],
        out_specs=whole_block,
        scratch_shapes=[pltpu.VMEM((slots + 1, width, width), F32)],
        compiler_params=pltpu.CompilerParams(vmem_limit_bytes=32 * 1024 * 1024),
    )(labels, incoming, base[0])
    return result[None]


def solution(mesh):
    placed = (
        P("sub", None, None, None),
        P("sub", None, None, None),
        P("sub", None, "tile"),
        P("sub", None, "tile"),
        P("sub", None, "tile"),
        P("sub", "tile", None, None),
    )
    return jax.shard_map(
        shards, mesh=mesh, in_specs=placed, out_specs=P("sub", "tile", None, None), check_vma=False
    )
```

```python
import functools

import jax
import jax.numpy as jnp
from jax import lax
from jax.experimental import pallas as pl
from jax.experimental.pallas import tpu as pltpu
from jax.sharding import PartitionSpec as P

MESH = pl.DeviceIdType.MESH
F32 = jnp.float32
BF16 = jnp.bfloat16


def exchange_kernel(
    dims,
    meta_sm,
    meta_any,
    coupling_hbm,
    inverse_hbm,
    cols_hbm,
    incoming,
    metas,
    labels,
    coupling,
    inverse,
    cols,
    target,
    held,
    total,
    packed,
    table,
    meta_all,
    load_sem,
    own_send,
    own_recv,
    relay_send,
    relay_recv,
    out_send,
    out_recv,
    meta_send,
    meta_recv,
    local_sem,
):
    n_sub, n_tile, panels, width, col_tiles, tile_count, capacity, slots = dims
    me = lax.axis_index("sub")
    col = lax.axis_index("tile")
    half_tile = n_tile // 2
    partner = col + 1 - 2 * (col % 2)
    across = (col + half_tile) % n_tile
    corner = (partner + half_tile) % n_tile
    places = (col, partner, across, corner)
    half = n_sub // 2
    side = me // half
    within = me % half

    def far_peer(j):
        return ((side + 1) % 2) * half + (within + j) % half

    def near_peer(j):
        return side * half + (within + j) % half

    loads = [
        pltpu.make_async_copy(cols_hbm.at[0], cols.at[0], load_sem.at[0]),
        pltpu.make_async_copy(inverse_hbm.at[0], inverse.at[0], load_sem.at[1]),
        pltpu.make_async_copy(coupling_hbm, coupling, load_sem.at[2]),
        pltpu.make_async_copy(
            inverse_hbm.at[pl.ds(1, panels - 1)], inverse.at[pl.ds(1, panels - 1)], load_sem.at[3]
        ),
        pltpu.make_async_copy(
            cols_hbm.at[pl.ds(1, panels - 1)], cols.at[pl.ds(1, panels - 1)], load_sem.at[4]
        ),
    ]
    for load in loads:
        load.start()

    barrier = pltpu.get_barrier_semaphore()
    for place in (partner, across):
        pl.semaphore_signal(barrier, inc=1, device_id={"tile": place}, device_id_type=MESH)

    @pl.loop(1, n_sub)
    def _(j):
        pl.semaphore_signal(
            barrier, inc=1, device_id={"sub": (me + j) % n_sub}, device_id_type=MESH
        )

    def solve_panel(k):
        target[...] = cols[k].astype(F32)
        start = k * (k - 1) // 2
        for m in range(k):
            target[...] -= jnp.dot(coupling[start + m], held[m], preferred_element_type=F32)
        inv = inverse[k]
        inv_high = inv.astype(BF16)
        inv_low = (inv - inv_high.astype(F32)).astype(BF16)
        value = target[...]
        high = value.astype(BF16)
        low = (value - high.astype(F32)).astype(BF16)
        answer = jnp.dot(inv_high, low, preferred_element_type=F32)
        answer += jnp.dot(inv_low, high, preferred_element_type=F32)
        answer += jnp.dot(inv_high, high, preferred_element_type=F32)
        held[k] = answer.astype(BF16)

    def own_copy(k, way):
        return pltpu.make_async_remote_copy(
            src_ref=held.at[k],
            dst_ref=held.at[(way + 1) * panels + k],
            send_sem=own_send.at[way, k],
            recv_sem=own_recv.at[way, k],
            device_id={"tile": (partner, across)[way]},
            device_id_type=MESH,
        )

    def relay_copy(k):
        return pltpu.make_async_remote_copy(
            src_ref=held.at[2 * panels + k],
            dst_ref=held.at[3 * panels + k],
            send_sem=relay_send.at[k],
            recv_sem=relay_recv.at[k],
            device_id={"tile": partner},
            device_id_type=MESH,
        )

    def out_copy(peer, source):
        return pltpu.make_async_remote_copy(
            src_ref=packed.at[peer],
            dst_ref=incoming.at[source],
            send_sem=out_send.at[peer],
            recv_sem=out_recv.at[source],
            device_id={"sub": peer},
            device_id_type=MESH,
        )

    def meta_copy(peer, source):
        return pltpu.make_async_remote_copy(
            src_ref=meta_any,
            dst_ref=metas.at[source],
            send_sem=meta_send.at[peer],
            recv_sem=meta_recv.at[source],
            device_id={"sub": peer},
            device_id_type=MESH,
        )

    loads[0].wait()
    loads[1].wait()
    solve_panel(0)
    pl.semaphore_wait(barrier, n_sub + 1)
    own_copy(0, 1).start()
    own_copy(0, 0).start()
    for load in loads[2:]:
        load.wait()
    for k in range(1, panels):
        solve_panel(k)
        own_copy(k, 1).start()
        own_copy(k, 0).start()

    @pl.loop(1, n_sub)
    def _(j):
        meta_copy((me + j) % n_sub, me).start()

    per_place = col_tiles * col_tiles

    def gram(u, k, first=False):
        right = held[k]
        for i in range(col_tiles):
            left = held[u * panels + k, :, i * width : (i + 1) * width]
            product = lax.dot_general(
                left, right, (((0,), (0,)), ((), ())), preferred_element_type=F32
            )
            for j in range(col_tiles):
                piece = product[:, j * width : (j + 1) * width]
                at = places[u] * per_place + i * col_tiles + j
                if first:
                    total[at] = piece
                else:
                    total[at] += piece

    def pick(read, low, default, value_of, store):
        def body(i, carry):
            count, chosen = carry
            value = read(i)
            hit = (value >= low) & (value < low + slots)
            new = value_of(i, value)
            chosen = tuple(
                jnp.where(hit & (count == r), new, c) for r, c in enumerate(chosen)
            )
            return count + jnp.where(hit, 1, 0), chosen

        start = (jnp.int32(0), tuple(jnp.int32(default) for _ in range(capacity)))
        _, chosen = lax.fori_loop(0, tile_count, body, start)
        for r, c in enumerate(chosen):
            store(r, c)

    @pl.loop(0, n_sub)
    def _(d):
        def store(r, c):
            table[d * capacity + r] = c

        pick(lambda i: meta_sm[0, i], d * slots, 0, lambda i, v: i, store)

    gram(0, 0, first=True)

    @pl.loop(1, panels)
    def _(k):
        gram(0, k)

    own_copy(0, 0).wait_recv()
    gram(1, 0, first=True)

    @pl.loop(1, panels)
    def _(k):
        own_copy(k, 0).wait_recv()
        gram(1, k)

    def remote_step(k, first):
        own_copy(k, 1).wait_recv()
        relay_copy(k).start()
        gram(2, k, first)
        relay_copy(k).wait_recv()
        gram(3, k, first)

    remote_step(0, True)

    @pl.loop(1, panels)
    def _(k):
        remote_step(k, False)

    def pack(d):
        for r in range(capacity):
            packed[d, r] = (-total[table[d * capacity + r]]).astype(BF16)

    @pl.loop(0, half)
    def _(j):
        pack(far_peer(j))
        out_copy(far_peer(j), me).start()

    @pl.loop(1, half)
    def _(j):
        pack(near_peer(j))
        out_copy(near_peer(j), me).start()

    pack(me)
    keep = pltpu.make_async_copy(packed.at[me], incoming.at[me], local_sem.at[0])
    keep.start()

    own_meta = pltpu.make_async_copy(meta_any, meta_all.at[me], local_sem.at[1])
    own_meta.start()

    @pl.loop(1, n_sub)
    def _(j):
        source = (me + j) % n_sub
        meta_copy(source, source).wait_recv()
        fetch = pltpu.make_async_copy(metas.at[source], meta_all.at[source], local_sem.at[2])
        fetch.start()
        fetch.wait()

    own_meta.wait()

    @pl.loop(0, n_sub)
    def _(s):
        def store(r, c):
            labels[s * capacity + r] = c

        pick(
            lambda i: meta_all[s, 0, i], me * slots, slots, lambda i, v: v - me * slots, store
        )

    @pl.loop(0, panels)
    def _(k):
        own_copy(k, 0).wait_send()
        own_copy(k, 1).wait_send()
        relay_copy(k).wait_send()

    @pl.loop(1, n_sub)
    def _(j):
        source = (me + j) % n_sub
        meta_copy(source, source).wait_send()
        out_copy(source, source).wait_send()
        out_copy(source, source).wait_recv()

    keep.wait()


def add_kernel(slots, capacity, labels, incoming, base, result, total):
    step = pl.program_id(0)

    @pl.when(step == 0)
    def _():
        total[pl.ds(0, slots)] = base[...].astype(F32)

    for r in range(capacity):
        total[labels[step * capacity + r]] += incoming[0, r].astype(F32)

    @pl.when(step == pl.num_programs(0) - 1)
    def _():
        result[...] = total[pl.ds(0, slots)].astype(BF16)


def shards(coupling, panel_inv, a_ib, owner, slot, base):
    lower_blocks = coupling[0]
    inverse = panel_inv[0]
    panels, width = inverse.shape[:2]
    col_count = a_ib.shape[2]
    right_cols = a_ib[0].reshape(panels, width, col_count)
    n_sub = lax.axis_size("sub")
    n_tile = lax.axis_size("tile")
    assert n_tile == 4 and n_sub % 2 == 0
    col_tiles = col_count // width
    tile_count = owner.shape[1] * owner.shape[2]
    assert owner.shape[1] == n_tile * col_tiles
    capacity = (tile_count + n_sub - 1) // n_sub
    slots = base.shape[1]
    room = (tile_count + 127) // 128 * 128
    meta = (owner[0] * slots + slot[0]).reshape(1, tile_count)
    meta = jnp.pad(meta, ((0, 0), (0, room - tile_count)))
    dims = (n_sub, n_tile, panels, width, col_tiles, tile_count, capacity, slots)
    any_spec = pl.BlockSpec(memory_space=pl.ANY)
    smem_spec = pl.BlockSpec(memory_space=pltpu.SMEM)
    dma = pltpu.SemaphoreType.DMA
    incoming, _, labels = pl.pallas_call(
        functools.partial(exchange_kernel, dims),
        out_shape=(
            jax.ShapeDtypeStruct((n_sub, capacity, width, width), BF16),
            jax.ShapeDtypeStruct((n_sub, 1, room), jnp.int32),
            jax.ShapeDtypeStruct((n_sub * capacity,), jnp.int32),
        ),
        in_specs=[smem_spec, any_spec, any_spec, any_spec, any_spec],
        out_specs=(any_spec, any_spec, smem_spec),
        scratch_shapes=[
            pltpu.VMEM(lower_blocks.shape, BF16),
            pltpu.VMEM(inverse.shape, F32),
            pltpu.VMEM(right_cols.shape, BF16),
            pltpu.VMEM((width, col_count), F32),
            pltpu.VMEM((n_tile * panels, width, col_count), BF16),
            pltpu.VMEM((tile_count, width, width), F32),
            pltpu.VMEM((n_sub, capacity, width, width), BF16),
            pltpu.SMEM((n_sub * capacity,), jnp.int32),
            pltpu.SMEM((n_sub, 1, room), jnp.int32),
            dma((5,)),
            dma((2, panels)),
            dma((2, panels)),
            dma((panels,)),
            dma((panels,)),
            dma((n_sub,)),
            dma((n_sub,)),
            dma((n_sub,)),
            dma((n_sub,)),
            dma((3,)),
        ],
        compiler_params=pltpu.CompilerParams(
            collective_id=0, has_side_effects=True, vmem_limit_bytes=60 * 1024 * 1024
        ),
    )(meta, meta, lower_blocks, inverse, right_cols)

    whole_block = pl.BlockSpec((slots, width, width), lambda s: (0, 0, 0))
    result = pl.pallas_call(
        functools.partial(add_kernel, slots, capacity),
        grid=(n_sub,),
        out_shape=jax.ShapeDtypeStruct((slots, width, width), BF16),
        in_specs=[
            smem_spec,
            pl.BlockSpec((1, capacity, width, width), lambda s: (s, 0, 0, 0)),
            whole_block,
        ],
        out_specs=whole_block,
        scratch_shapes=[pltpu.VMEM((slots + 1, width, width), F32)],
        compiler_params=pltpu.CompilerParams(vmem_limit_bytes=62 * 1024 * 1024),
    )(labels, incoming, base[0])
    return result[None]


def solution(mesh):
    placed = (
        P("sub", None, None, None),
        P("sub", None, None, None),
        P("sub", None, "tile"),
        P("sub", None, "tile"),
        P("sub", None, "tile"),
        P("sub", "tile", None, None),
    )
    return jax.shard_map(
        shards, mesh=mesh, in_specs=placed, out_specs=P("sub", "tile", None, None), check_vma=False
    )
```
